32 devices in a mesh: grp: 2 (over y), ia: 4 (over z), ja: 4 (over x, core).
Axes of the slice: x: 2, y: 2, z: 4, core: 2. Of those that a mesh axis runs over, the one named last changes fastest.
Arguments:
- doubles: bfloat16 [8, 16, 384, 384], P(('grp', 'ia'), 'ja'), parts along dimension 0, may hold values from -6 to 6
- aux_factors: bfloat16 [4, 384, 384], P('ia'), may hold values from -0.15625 to 0.15625
- cycle_factors: bfloat16 [16, 384, 128], replicated, may hold values from -0.21875 to 0.21875
Outputs:
- sigma: bfloat16 [8, 16, 384, 384], P(('grp', 'ia'), 'ja'), parts along dimension 0
The draws below stay inside these ranges and needn't reach their ends.
There are 2 independent parts, one for each index of `grp`. The reference program is written for one: setup_inputs(seed, part) draws one part's arguments, and reference() takes and returns one part's arrays. A program takes and returns all parts, laid end to end along the dimension named above; an argument that names none is the same for every part. Nothing has to cross between parts.
All inputs are finite; a program needn't handle non-finite values.
Results may differ from the reference program's by a relative error of at most 0.008.
Values may be sent and summed in bfloat16 or wider, within the bound.
A program may use at most 128 MiB of HBM per device.

```python
import jax
import jax.numpy as jnp
from jax import lax

V = 384
Q = 128
AUX = 4
OI = 4
J_ALL = 16


def block_scale(rng, dims, split, low, high):
    loudness = 1.0
    for dim, shards_of in split:
        draws = jax.random.uniform(jax.random.fold_in(jax.random.fold_in(rng, 6), dim), (shards_of,), jnp.float32, low / len(split), high / len(split))
        loudness = loudness * jnp.repeat(jnp.exp(draws), dims[dim] // shards_of).reshape((-1,) + (1,) * (len(dims) - 1 - dim))
    return loudness


def noise(own_key, dims, spread, reach, shards=(), held_as=jnp.bfloat16):
    result = jax.random.normal(own_key, dims, jnp.float32) * spread
    if len(shards) > 0:
        result = block_scale(own_key, dims, shards, -0.22, 0.18) * result
    return jnp.clip(result, min=-reach, max=reach).astype(held_as)


def setup_inputs(seed: int = 0, part: int = 0) -> dict:
    streams_of = jax.random.split(jax.random.key(seed), 4)
    own_keys = jax.random.split(jax.random.fold_in(streams_of[3], part), 4)
    doubles = noise(own_keys[0], (OI, J_ALL, V, V), 1.0, 6.0, ((0, 4), (1, 4)))
    aux_factors = noise(streams_of[1], (AUX, V, V), (V * 4) ** -0.5, 0.15625, ((0, 4),))
    cycle_factors = noise(streams_of[2], (J_ALL, V, Q), (J_ALL * V // 8) ** -0.5, 0.21875)
    return dict(doubles=doubles, aux_factors=aux_factors, cycle_factors=cycle_factors)


def ladder_terms(pair_blocks, factor):
    wide_pairs = pair_blocks.astype(jnp.float32)
    wide_factor = factor.astype(jnp.float32)
    halfway = jnp.einsum('pcd,bd->pcb', wide_pairs, wide_factor).astype(jnp.bfloat16)
    return jnp.einsum('ac,pcb->pab', wide_factor, halfway.astype(jnp.float32))


def reference(doubles, aux_factors, cycle_factors):
    pair_blocks = doubles.reshape(OI * J_ALL, V, V)

    def one_step(position, running):
        factor = lax.dynamic_index_in_dim(aux_factors, position, 0, keepdims=False)
        return running + ladder_terms(pair_blocks, factor)

    ladder = lax.fori_loop(0, AUX, one_step, jnp.zeros((OI * J_ALL, V, V), jnp.float32))
    ladder = ladder.reshape(OI, J_ALL, V, V)
    wide_cycle = cycle_factors.astype(jnp.float32)
    latent = jnp.einsum('ijab,jbq->iaq', doubles.astype(jnp.float32), wide_cycle).astype(jnp.bfloat16)
    cycle_term = jnp.einsum('iaq,jbq->ijab', latent.astype(jnp.float32), wide_cycle).astype(jnp.bfloat16)
    return (ladder + cycle_term.astype(jnp.float32)).astype(jnp.bfloat16)
```

```python
import functools

import jax
import jax.numpy as jnp
from jax import lax
from jax.experimental import pallas as pl
from jax.experimental.pallas import tpu as pltpu
from jax.sharding import PartitionSpec as P

MESH = pl.DeviceIdType.MESH
F32 = jnp.float32
BF16 = jnp.bfloat16
NT = (((1,), (1,)), ((), ()))
CORES = 2
LAST_STAGE = 4


def sigma_kernel(n, nj, ny, d_hbm, aux_hbm, u_hbm, out, d, u, aux, half, acc,
                 plat, lat_own, lat_sib, lat_in, lat, load_sem, d_sem,
                 z_ready, x_ready, y_ready, s_ready, z_send, z_recv, r_send, r_recv,
                 s_send, s_recv, p_send, p_recv, l_send, l_recv):
    nx = nj // CORES
    pairs_j, width, _ = d.shape
    rows = width // (ny * nj)
    lat_rows = width // CORES
    iz = lax.axis_index("ia")
    iy = lax.axis_index("grp") if ny > 1 else 0
    ij = lax.axis_index("ja")
    core = ij % CORES
    sibling = {"ja": ij ^ 1}
    spots = [(y, x) for y in range(ny) for x in range(nx)]
    direct = [0] + [m for m, (y, x) in enumerate(spots) if y > 0 and x > 0]
    relayed = [m for m in range(1, len(spots)) if m not in direct]

    def piece(m, base):
        y, x = spots[m]
        owner = (iy ^ y) * nj + (base ^ (CORES * x))
        return pl.ds(pl.multiple_of(owner * rows, rows), rows)

    def lat_half(c):
        return pl.ds(pl.multiple_of(c * lat_rows, lat_rows), lat_rows)

    def plane(m):
        y, x = spots[m]
        return {"grp": iy ^ y} if x == 0 else {"ja": ij ^ (CORES * x)}

    load_aux = pltpu.make_async_copy(aux_hbm.at[0], aux.at[0], load_sem.at[0])
    load_u = pltpu.make_async_copy(
        u_hbm.at[pl.ds(ij * pairs_j, pairs_j)], u, load_sem.at[1])

    def load_d(j):
        return pltpu.make_async_copy(d_hbm.at[0, j], d.at[j], d_sem.at[j])

    load_u.start()
    for j in range(pairs_j):
        load_d(j).start()
    load_aux.start()

    def remote(src, dst, send, recv, where):
        return pltpu.make_async_remote_copy(
            src_ref=src, dst_ref=dst, send_sem=send, recv_sem=recv,
            device_id=where, device_id_type=MESH)

    def z_copy(k, m, src=aux.at[0]):
        return remote(src.at[piece(m, ij)], aux.at[k, piece(m, ij)],
                      z_send.at[k - 1], z_recv.at[(k - 1) * len(direct) + direct.index(m)],
                      {"ia": iz ^ k})

    def r_copy(k, m, from_m=0):
        part = aux.at[k, piece(from_m, ij)]
        return remote(part, part, r_send.at[k - 1],
                      r_recv.at[(k - 1) * len(relayed) + relayed.index(m)], plane(m))

    def s_copy(k, m, base):
        part = aux.at[k, piece(m, base)]
        return remote(part, part, s_send.at[k - 1], s_recv.at[k - 1], sibling)

    def sent(k, count, sem):
        part = aux.at[k, pl.ds(0, count * rows)]
        return pltpu.make_async_copy(part, part, sem.at[k - 1])

    def p_copy(x):
        if x == 0:
            return remote(plat, lat_sib, p_send.at[0], p_recv.at[0], sibling)
        return remote(plat.at[lat_half(core)], lat_in.at[x], p_send.at[x], p_recv.at[x],
                      {"ja": ij ^ (CORES * x)})

    def l_copy(c):
        return remote(lat.at[lat_half(c)], lat.at[lat_half(c)], l_send, l_recv, sibling)

    def signal(sem, where):
        pl.semaphore_signal(sem, inc=1, device_id=where, device_id_type=MESH)

    partners = [(iz ^ k, iz, {"ia": iz ^ k}, z_ready.at[k]) for k in range(1, n)]
    partners += [(ij ^ (CORES * x), ij, {"ja": ij ^ (CORES * x)}, x_ready.at[x])
                 for x in range(1, nx)]
    partners += [(ij ^ 1, ij, sibling, s_ready)]
    partners += [(iy ^ y, iy, {"grp": iy ^ y}, y_ready.at[y]) for y in range(1, ny)]

    barrier = pltpu.get_barrier_semaphore()
    for other, me, where, _ in partners:
        @pl.when(other > me)
        def _():
            signal(barrier, where)
    lower = iz + ij // CORES + core + iy

    @pl.when(lower > 0)
    def _():
        pl.semaphore_wait(barrier, lower)

    def await_ready(index):
        other, me, _, ready = partners[index]

        @pl.when(other > me)
        def _():
            pl.semaphore_wait(ready, 1)

    def send_down(stage):
        for t in range(n - 1):
            for near in (True, False):
                turns = [m for m in direct
                         if min(min(t + 1, 2) if near else t + 1 + (m > 0), LAST_STAGE) == stage]
                if turns:
                    @pl.when(t == iz - 1 if near else t < iz - 1)
                    def _():
                        for m in turns:
                            z_copy(iz ^ t, m, aux_hbm.at[0] if stage == 1 else aux.at[0]).start()

    def send_up(first, near, who):
        for t in range(1, n):
            turns = direct[:1] if first else direct[1:]
            if first and near:
                turns = direct
            @pl.when((t == iz + 1 if near else t > iz + 1) & who)
            def _():
                if first:
                    pl.semaphore_wait(z_ready.at[iz ^ t], 1)
                for m in turns:
                    z_copy(iz ^ t, m).start()

    send_down(1)
    for other, me, where, ready in partners:
        @pl.when(other < me)
        def _():
            signal(ready, where)

    with jax.named_scope("latent"):
        load_u.wait()
        total = jnp.zeros(lat_own.shape, F32)
        for j in range(pairs_j):
            load_d(j).wait()
            total += jnp.dot(d[j], u[j], preferred_element_type=F32)
        lat_own[...] = total
        plat[...] = total.astype(BF16)

    load_aux.wait()
    send_down(2)
    send_up(True, True, iz > 0)

    def halfway(k, place):
        for j in range(pairs_j):
            block = lax.dot_general(d[j], aux[k], NT, preferred_element_type=F32)
            half[place * width:(place + 1) * width,
                 j * width:(j + 1) * width] = block.astype(BF16)

    def ladder(k):
        return jnp.dot(aux[k], half[:width, :], preferred_element_type=F32)

    def finish(ks):
        left = jnp.concatenate([aux[k] for k in ks] + [lat[...]], axis=1)
        res = jnp.dot(left, half[(2 - len(ks)) * width:, :], preferred_element_type=F32)
        if n > 1:
            res += acc[...]
        for j in range(pairs_j):
            out[0, j] = res[:, j * width:(j + 1) * width].astype(BF16)

    for j in range(pairs_j):
        half[2 * width:, j * width:(j + 1) * width] = u[j].T

    with jax.named_scope("own"):
        halfway(0, 0 if n > 1 else 1)
    send_down(3)
    send_up(True, True, iz == 0)
    send_up(True, False, iz > 0)
    for index in range(n - 1, len(partners)):
        await_ready(index)
    p_copy(0).start()
    with jax.named_scope("ownlad"):
        if n > 1:
            acc[...] = ladder(0)
    send_down(4)
    with jax.named_scope("up"):
        send_up(True, False, iz == 0)

    def pass_on(k):
        with jax.named_scope("pass%d" % k):
            z_copy(k, 0).wait_recv()
            for m in relayed:
                r_copy(k, m).start()
            s_copy(k, 0, ij).start()

    def share(k):
        with jax.named_scope("shareA%d" % k):
            for m in direct[1:]:
                z_copy(k, m).wait_recv()
                s_copy(k, m, ij).start()
        with jax.named_scope("shareB%d" % k):
            for m in relayed:
                r_copy(k, m, m).wait_recv()
                s_copy(k, m, ij).start()

    def complete(k):
        with jax.named_scope("compl%d" % k):
            sent(k, len(spots), s_recv).wait()

    def chip_latent():
        p_copy(0).wait_recv()
        lat_own[...] += lat_sib[...].astype(F32)
        p_copy(0).wait_send()
        plat[...] = lat_own[...].astype(BF16)

    def cross_latent():
        for x in range(1, nx):
            p_copy(x).start()

    def whole_latent():
        with jax.named_scope("wholelat"):
            mine = lat_own[lat_half(core), :]
            for x in range(1, nx):
                p_copy(x).wait_recv()
                mine += lat_in[x].astype(F32)
            lat[lat_half(core), :] = mine.astype(BF16)

    chip_latent()
    if n > 1:
        pass_on(1)
    send_up(False, False, iz >= 0)
    for k in range(2, min(4, n)):
        pass_on(k)
    cross_latent()
    for k in range(1, min(2, n)):
        share(k)
    last = list(range(max(n - 2, min(n - 1, 1)), n))
    for k in range(1, last[0]):
        complete(k)
        with jax.named_scope("half%d" % k):
            halfway(k, 0)
        share(k + 1)
        if k + 3 < n:
            pass_on(k + 3)
        with jax.named_scope("lad%d" % k):
            acc[...] += ladder(k)
    whole_latent()
    l_copy(core).start()
    for place, k in enumerate(last):
        if place == 0 and len(last) > 1:
            share(last[1])
        if k > 0:
            complete(k)
            with jax.named_scope("half%d" % k):
                halfway(k, 2 - len(last) + place)
    l_copy(core ^ 1).wait_recv()
    with jax.named_scope("final"):
        finish(last)

    with jax.named_scope("tail"):
        for k in range(1, n):
            sent(k, len(direct), z_send).wait()
            if relayed:
                sent(k, len(relayed), r_send).wait()
            sent(k, len(spots), s_send).wait()
        for x in range(1, nx):
            p_copy(x).wait_send()
        l_copy(core).wait_send()


def shards(n, nj, grps, doubles, aux_factors, cycle_factors):
    _, pairs_j, width, _ = doubles.shape
    rank = cycle_factors.shape[2]
    nx = nj // CORES
    ny = grps if width % (grps * nj * 16) == 0 else 1
    others = max(n - 1, 1)
    ahead = 1 + (nx - 1) * (ny - 1)
    dma = pltpu.SemaphoreType.DMA
    flag = pltpu.SemaphoreType.REGULAR
    hbm = pl.BlockSpec(memory_space=pltpu.HBM)
    flops = 4 * n * pairs_j * width**3 + 4 * pairs_j * width * width * rank
    return pl.pallas_call(
        functools.partial(sigma_kernel, n, nj, ny),
        out_shape=pltpu.VMEM(doubles.shape, BF16),
        in_specs=[hbm] * 3,
        out_specs=pl.BlockSpec(memory_space=pltpu.VMEM),
        scratch_shapes=[
            pltpu.VMEM((pairs_j, width, width), BF16),
            pltpu.VMEM((pairs_j, width, rank), BF16),
            pltpu.VMEM((n, width, width), BF16),
            pltpu.VMEM((2 * width + rank, pairs_j * width), BF16),
            pltpu.VMEM((width, pairs_j * width), F32),
            pltpu.VMEM((width, rank), BF16),
            pltpu.VMEM((width, rank), F32),
            pltpu.VMEM((width, rank), BF16),
            pltpu.VMEM((nx, width // CORES, rank), BF16),
            pltpu.VMEM((width, rank), BF16),
            dma((2,)), dma((pairs_j,)),
            flag((n,)), flag((nx,)), flag((ny,)), flag,
            dma((others,)), dma((others * ahead,)),
            dma((others,)), dma((others * max(nx * ny - ahead, 1),)),
            dma((others,)), dma((others,)),
            dma((nx,)), dma((nx,)),
            dma, dma,
        ],
        compiler_params=pltpu.CompilerParams(
            collective_id=0, has_side_effects=True, vmem_limit_bytes=67043328 - doubles.size * 2 - 2**16),
        cost_estimate=pl.CostEstimate(
            flops=flops, bytes_accessed=4 * doubles.size, transcendentals=0),
    )(doubles, aux_factors, cycle_factors)


def solution(mesh):
    in_specs = (P(("grp", "ia"), "ja", None, None), P("ia", None, None), P())
    out_specs = P(("grp", "ia"), "ja", None, None)
    body = functools.partial(shards, mesh.shape["ia"], mesh.shape["ja"], mesh.shape["grp"])
    return jax.shard_map(body, mesh=mesh, in_specs=in_specs, out_specs=out_specs, check_vma=False)
```

```python
import functools

import jax
import jax.numpy as jnp
from jax import lax
from jax.experimental import pallas as pl
from jax.experimental.pallas import tpu as pltpu
from jax.sharding import PartitionSpec as P

MESH = pl.DeviceIdType.MESH
F32 = jnp.float32
BF16 = jnp.bfloat16
NT = (((1,), (1,)), ((), ()))
CORES = 2
LAST_STAGE = 5
SPLIT = 1


def sigma_kernel(n, nj, ny, d_hbm, aux_hbm, u_hbm, out, d, u, aux, half, acc,
                 plat, lat_own, lat_sib, lat_in, lat, load_sem, d_sem,
                 z_ready, x_ready, y_ready, s_ready, z_send, z_recv, r_send, r_recv,
                 s_send, s_recv, p_send, p_recv, l_send, l_recv):
    nx = nj // CORES
    pairs_j, width, _ = d.shape
    rows = width // (ny * nj)
    lat_rows = width // CORES
    iz = lax.axis_index("ia")
    iy = lax.axis_index("grp") if ny > 1 else 0
    ij = lax.axis_index("ja")
    core = ij % CORES
    sibling = {"ja": ij ^ 1}
    spots = [(y, x) for y in range(ny) for x in range(nx)]
    direct = [0] + [m for m, (y, x) in enumerate(spots) if y > 0 and x > 0]
    relayed = [m for m in range(1, len(spots)) if m not in direct]

    def piece(m, base):
        y, x = spots[m]
        owner = (iy ^ y) * nj + (base ^ (CORES * x))
        return pl.ds(pl.multiple_of(owner * rows, rows), rows)

    def lat_half(c):
        return pl.ds(pl.multiple_of(c * lat_rows, lat_rows), lat_rows)

    def plane(m):
        y, x = spots[m]
        return {"grp": iy ^ y} if x == 0 else {"ja": ij ^ (CORES * x)}

    load_aux = pltpu.make_async_copy(aux_hbm.at[0], aux.at[0], load_sem.at[0])
    load_u = pltpu.make_async_copy(
        u_hbm.at[pl.ds(ij * pairs_j, pairs_j)], u, load_sem.at[1])

    def load_d(j, part):
        share_of = pl.ds(part * (width // SPLIT), width // SPLIT)
        return pltpu.make_async_copy(d_hbm.at[0, j, share_of], d.at[j, share_of],
                                     d_sem.at[j])

    orders = [sorted(range(1, n), key=lambda k: (abs((z ^ k) - z) if z ^ k < z else n, k)) for z in range(n)]
    order = [0] + [sum(jnp.where(iz == z, orders[z][i], 0) for z in range(n))
                   for i in range(n - 1)]

    load_u.start()
    for j in range(pairs_j):
        for part in range(SPLIT):
            load_d(j, part).start()
    load_aux.start()

    def remote(src, dst, send, recv, where):
        return pltpu.make_async_remote_copy(
            src_ref=src, dst_ref=dst, send_sem=send, recv_sem=recv,
            device_id=where, device_id_type=MESH)

    def z_copy(k, m, src=aux.at[0]):
        return remote(src.at[piece(m, ij)], aux.at[k, piece(m, ij)],
                      z_send.at[k - 1], z_recv.at[(k - 1) * len(direct) + direct.index(m)],
                      {"ia": iz ^ k})

    def r_copy(k, m, from_m=0):
        part = aux.at[k, piece(from_m, ij)]
        return remote(part, part, r_send.at[k - 1],
                      r_recv.at[(k - 1) * len(relayed) + relayed.index(m)], plane(m))

    def s_copy(k, m, base):
        part = aux.at[k, piece(m, base)]
        return remote(part, part, s_send.at[k - 1], s_recv.at[k - 1], sibling)

    def sent(k, count, sem):
        part = aux.at[k, pl.ds(0, count * rows)]
        return pltpu.make_async_copy(part, part, sem.at[k - 1])

    def p_copy(x):
        if x == 0:
            return remote(plat, lat_sib, p_send.at[0], p_recv.at[0], sibling)
        return remote(plat.at[lat_half(core)], lat_in.at[x], p_send.at[x], p_recv.at[x],
                      {"ja": ij ^ (CORES * x)})

    def l_copy(c):
        return remote(lat.at[lat_half(c)], lat.at[lat_half(c)], l_send, l_recv, sibling)

    def signal(sem, where):
        pl.semaphore_signal(sem, inc=1, device_id=where, device_id_type=MESH)

    partners = [(iz ^ k, iz, {"ia": iz ^ k}, z_ready.at[k]) for k in range(1, n)]
    partners += [(ij ^ (CORES * x), ij, {"ja": ij ^ (CORES * x)}, x_ready.at[x])
                 for x in range(1, nx)]
    partners += [(ij ^ 1, ij, sibling, s_ready)]
    partners += [(iy ^ y, iy, {"grp": iy ^ y}, y_ready.at[y]) for y in range(1, ny)]

    barrier = pltpu.get_barrier_semaphore()
    for other, me, where, _ in partners:
        @pl.when(other > me)
        def _():
            signal(barrier, where)
    lower = iz + ij // CORES + core + iy

    @pl.when(lower > 0)
    def _():
        pl.semaphore_wait(barrier, lower)

    def await_ready(index):
        other, me, _, ready = partners[index]

        @pl.when(other > me)
        def _():
            pl.semaphore_wait(ready, 1)

    def stage_of(t, m, near):
        if t == 0:
            return 1 + (m > 0) * (0 if near else 2)
        return 3 if near else t + 2 + (m > 0)

    def send_down(stage):
        for t in range(n - 1):
            for near in (True, False):
                turns = [m for m in direct
                         if min(stage_of(t, m, near), LAST_STAGE) == stage]
                if turns:
                    @pl.when(t == iz - 1 if near else t < iz - 1)
                    def _():
                        for m in turns:
                            z_copy(iz ^ t, m, aux_hbm.at[0] if stage < 3 else aux.at[0]).start()

    def send_up(first, near, who):
        for t in range(1, n):
            turns = direct[:1] if first else direct[1:]
            if first and near:
                turns = direct
            @pl.when((t == iz + 1 if near else t > iz + 1) & who)
            def _():
                if first:
                    pl.semaphore_wait(z_ready.at[iz ^ t], 1)
                for m in turns:
                    z_copy(iz ^ t, m).start()

    send_down(1)
    for other, me, where, ready in partners:
        @pl.when(other < me)
        def _():
            signal(ready, where)

    with jax.named_scope("latent"):
        load_u.wait()
        total = jnp.zeros(lat_own.shape, F32)
        for j in range(pairs_j):
            pltpu.make_async_copy(d_hbm.at[0, j], d.at[j], d_sem.at[j]).wait()
            if j == 0:
                send_down(2)
            total += jnp.dot(d[j], u[j], preferred_element_type=F32)
        lat_own[...] = total
        plat[...] = total.astype(BF16)

    load_aux.wait()
    send_down(3)
    send_up(True, True, iz > 0)

    def halfway(k, place, pairs):
        for j in pairs:
            block = lax.dot_general(d[j], aux[k], NT, preferred_element_type=F32)
            half[place * width:(place + 1) * width,
                 j * width:(j + 1) * width] = block.astype(BF16)

    def ladder(k, pairs, add):
        cols = slice(pairs[0] * width, (pairs[-1] + 1) * width)
        res = jnp.dot(aux[k], half[:width, cols], preferred_element_type=F32)
        acc[:, cols] = acc[:, cols] + res if add else res

    every = list(range(pairs_j))
    early, late = every[:(pairs_j + 1) // 2], every[(pairs_j + 1) // 2:] or every[-1:]

    def finish(ks):
        left = jnp.concatenate([aux[k] for k in ks] + [lat[...]], axis=1)
        res = jnp.dot(left, half[(2 - len(ks)) * width:, :], preferred_element_type=F32)
        if n > 1:
            res += acc[...]
        for j in range(pairs_j):
            out[0, j] = res[:, j * width:(j + 1) * width].astype(BF16)

    for j in range(pairs_j):
        half[2 * width:, j * width:(j + 1) * width] = u[j].T

    with jax.named_scope("own"):
        halfway(0, 0 if n > 1 else 1, every)
    send_down(4)
    send_up(True, True, iz == 0)
    send_up(True, False, iz > 0)
    for index in range(n - 1, len(partners)):
        await_ready(index)
    p_copy(0).start()
    with jax.named_scope("ownlad"):
        if n > 1:
            ladder(0, every, False)
    send_down(5)
    with jax.named_scope("up"):
        send_up(True, False, iz == 0)

    def pass_on(i):
        k = order[i]
        with jax.named_scope("pass%d" % i):
            z_copy(k, 0).wait_recv()
            for m in relayed:
                r_copy(k, m).start()
            s_copy(k, 0, ij).start()

    def share(i):
        k = order[i]
        with jax.named_scope("shareA%d" % i):
            for m in direct[1:]:
                z_copy(k, m).wait_recv()
                s_copy(k, m, ij).start()
        with jax.named_scope("shareB%d" % i):
            for m in relayed:
                r_copy(k, m, m).wait_recv()
                s_copy(k, m, ij).start()

    def complete(i):
        k = order[i]
        with jax.named_scope("compl%d" % i):
            sent(k, len(spots), s_recv).wait()

    def chip_latent():
        p_copy(0).wait_recv()
        lat_own[...] += lat_sib[...].astype(F32)
        p_copy(0).wait_send()
        plat[...] = lat_own[...].astype(BF16)

    def cross_latent():
        for x in range(1, nx):
            p_copy(x).start()

    def whole_latent():
        with jax.named_scope("wholelat"):
            mine = lat_own[lat_half(core), :]
            for x in range(1, nx):
                p_copy(x).wait_recv()
                mine += lat_in[x].astype(F32)
            lat[lat_half(core), :] = mine.astype(BF16)

    chip_latent()
    for i in range(1, min(2, n)):
        pass_on(i)
    send_up(False, False, iz >= 0)
    for i in range(2, min(4, n)):
        pass_on(i)
    cross_latent()
    for i in range(1, min(2, n)):
        share(i)
    last = list(range(max(n - 2, min(n - 1, 1)), n))
    for i in range(1, last[0]):
        complete(i)
        with jax.named_scope("halfA%d" % i):
            halfway(order[i], 0, early)
        share(i + 1)
        with jax.named_scope("halfB%d" % i):
            halfway(order[i], 0, late)
        if i + 3 < n:
            pass_on(i + 3)
        with jax.named_scope("ladA%d" % i):
            ladder(order[i], early, True)
        if i == last[0] - 1 and len(last) > 1:
            share(last[1])
        with jax.named_scope("ladB%d" % i):
            ladder(order[i], late, True)
    whole_latent()
    l_copy(core).start()
    if last[0] == 1 and len(last) > 1:
        share(last[1])
    for place, i in enumerate(last):
        if i > 0:
            complete(i)
            with jax.named_scope("half%d" % i):
                halfway(order[i], 2 - len(last) + place, every)
    l_copy(core ^ 1).wait_recv()
    with jax.named_scope("final"):
        finish([order[i] for i in last])

    with jax.named_scope("tail"):
        for k in range(1, n):
            sent(k, len(direct), z_send).wait()
            if relayed:
                sent(k, len(relayed), r_send).wait()
            sent(k, len(spots), s_send).wait()
        for x in range(1, nx):
            p_copy(x).wait_send()
        l_copy(core).wait_send()


def shards(n, nj, grps, doubles, aux_factors, cycle_factors):
    _, pairs_j, width, _ = doubles.shape
    rank = cycle_factors.shape[2]
    nx = nj // CORES
    ny = grps if width % (grps * nj * 16) == 0 else 1
    others = max(n - 1, 1)
    ahead = 1 + (nx - 1) * (ny - 1)
    dma = pltpu.SemaphoreType.DMA
    flag = pltpu.SemaphoreType.REGULAR
    hbm = pl.BlockSpec(memory_space=pltpu.HBM)
    flops = 4 * n * pairs_j * width**3 + 4 * pairs_j * width * width * rank
    return pl.pallas_call(
        functools.partial(sigma_kernel, n, nj, ny),
        out_shape=pltpu.VMEM(doubles.shape, BF16),
        in_specs=[hbm] * 3,
        out_specs=pl.BlockSpec(memory_space=pltpu.VMEM),
        scratch_shapes=[
            pltpu.VMEM((pairs_j, width, width), BF16),
            pltpu.VMEM((pairs_j, width, rank), BF16),
            pltpu.VMEM((n, width, width), BF16),
            pltpu.VMEM((2 * width + rank, pairs_j * width), BF16),
            pltpu.VMEM((width, pairs_j * width), F32),
            pltpu.VMEM((width, rank), BF16),
            pltpu.VMEM((width, rank), F32),
            pltpu.VMEM((width, rank), BF16),
            pltpu.VMEM((nx, width // CORES, rank), BF16),
            pltpu.VMEM((width, rank), BF16),
            dma((2,)), dma((pairs_j,)),
            flag((n,)), flag((nx,)), flag((ny,)), flag,
            dma((others,)), dma((others * ahead,)),
            dma((others,)), dma((others * max(nx * ny - ahead, 1),)),
            dma((others,)), dma((others,)),
            dma((nx,)), dma((nx,)),
            dma, dma,
        ],
        compiler_params=pltpu.CompilerParams(
            collective_id=0, has_side_effects=True, vmem_limit_bytes=67043328 - doubles.size * 2 - 2**16),
        cost_estimate=pl.CostEstimate(
            flops=flops, bytes_accessed=4 * doubles.size, transcendentals=0),
    )(doubles, aux_factors, cycle_factors)


def solution(mesh):
    in_specs = (P(("grp", "ia"), "ja", None, None), P("ia", None, None), P())
    out_specs = P(("grp", "ia"), "ja", None, None)
    body = functools.partial(shards, mesh.shape["ia"], mesh.shape["ja"], mesh.shape["grp"])
    return jax.shard_map(body, mesh=mesh, in_specs=in_specs, out_specs=out_specs, check_vma=False)
```

```python
import functools

import jax
import jax.numpy as jnp
from jax import lax
from jax.experimental import pallas as pl
from jax.experimental.pallas import tpu as pltpu
from jax.sharding import PartitionSpec as P

MESH = pl.DeviceIdType.MESH
F32 = jnp.float32
BF16 = jnp.bfloat16
NT = (((1,), (1,)), ((), ()))
CORES = 2
LAST_STAGE = 5
SPLIT = 1


def sigma_kernel(n, nj, ny, d_hbm, aux_hbm, u_hbm, out, d, u, aux, half, acc,
                 plat, lat_own, lat_sib, lat_in, lat, load_sem, d_sem,
                 z_ready, x_ready, y_ready, s_ready, z_send, z_recv, r_send, r_recv,
                 s_send, s_recv, p_send, p_recv, l_send, l_recv):
    nx = nj // CORES
    pairs_j, width, _ = d.shape
    rows = width // (ny * nj)
    lat_rows = width // CORES
    iz = lax.axis_index("ia")
    iy = lax.axis_index("grp") if ny > 1 else 0
    ij = lax.axis_index("ja")
    core = ij % CORES
    sibling = {"ja": ij ^ 1}
    spots = [(y, x) for y in range(ny) for x in range(nx)]
    direct = [0] + [m for m, (y, x) in enumerate(spots) if y > 0 and x > 0]
    relayed = [m for m in range(1, len(spots)) if m not in direct]

    def piece(m, base):
        y, x = spots[m]
        owner = (iy ^ y) * nj + (base ^ (CORES * x))
        return pl.ds(pl.multiple_of(owner * rows, rows), rows)

    def lat_half(c):
        return pl.ds(pl.multiple_of(c * lat_rows, lat_rows), lat_rows)

    def plane(m):
        y, x = spots[m]
        return {"grp": iy ^ y} if x == 0 else {"ja": ij ^ (CORES * x)}

    load_aux = pltpu.make_async_copy(aux_hbm.at[0], aux.at[0], load_sem.at[0])
    load_u = pltpu.make_async_copy(
        u_hbm.at[pl.ds(ij * pairs_j, pairs_j)], u, load_sem.at[1])

    def load_d(j, part):
        share_of = pl.ds(part * (width // SPLIT), width // SPLIT)
        return pltpu.make_async_copy(d_hbm.at[0, j, share_of], d.at[j, share_of],
                                     d_sem.at[j])

    orders = [sorted(range(1, n), key=lambda k: (abs((z ^ k) - z) if z ^ k < z else n, k)) for z in range(n)]
    order = [0] + [sum(jnp.where(iz == z, orders[z][i], 0) for z in range(n))
                   for i in range(n - 1)]

    load_u.start()
    for j in range(pairs_j):
        for part in range(SPLIT):
            load_d(j, part).start()
    load_aux.start()

    def remote(src, dst, send, recv, where):
        return pltpu.make_async_remote_copy(
            src_ref=src, dst_ref=dst, send_sem=send, recv_sem=recv,
            device_id=where, device_id_type=MESH)

    def z_copy(k, m, src=aux.at[0]):
        return remote(src.at[piece(m, ij)], aux.at[k, piece(m, ij)],
                      z_send.at[k - 1], z_recv.at[(k - 1) * len(direct) + direct.index(m)],
                      {"ia": iz ^ k})

    def r_copy(k, m, from_m=0):
        part = aux.at[k, piece(from_m, ij)]
        return remote(part, part, r_send.at[k - 1],
                      r_recv.at[(k - 1) * len(relayed) + relayed.index(m)], plane(m))

    def s_copy(k, m, base):
        part = aux.at[k, piece(m, base)]
        return remote(part, part, s_send.at[k - 1], s_recv.at[k - 1], sibling)

    def sent(k, count, sem):
        part = aux.at[k, pl.ds(0, count * rows)]
        return pltpu.make_async_copy(part, part, sem.at[k - 1])

    def p_copy(x):
        if x == 0:
            return remote(plat, lat_sib, p_send.at[0], p_recv.at[0], sibling)
        return remote(plat.at[lat_half(core)], lat_in.at[x], p_send.at[x], p_recv.at[x],
                      {"ja": ij ^ (CORES * x)})

    def l_copy(c):
        return remote(lat.at[lat_half(c)], lat.at[lat_half(c)], l_send, l_recv, sibling)

    def signal(sem, where):
        pl.semaphore_signal(sem, inc=1, device_id=where, device_id_type=MESH)

    partners = [(iz ^ k, iz, {"ia": iz ^ k}, z_ready.at[k]) for k in range(1, n)]
    partners += [(ij ^ (CORES * x), ij, {"ja": ij ^ (CORES * x)}, x_ready.at[x])
                 for x in range(1, nx)]
    partners += [(ij ^ 1, ij, sibling, s_ready)]
    partners += [(iy ^ y, iy, {"grp": iy ^ y}, y_ready.at[y]) for y in range(1, ny)]

    barrier = pltpu.get_barrier_semaphore()
    for other, me, where, _ in partners:
        @pl.when(other > me)
        def _():
            signal(barrier, where)
    lower = iz + ij // CORES + core + iy

    @pl.when(lower > 0)
    def _():
        pl.semaphore_wait(barrier, lower)

    def await_ready(index):
        other, me, _, ready = partners[index]

        @pl.when(other > me)
        def _():
            pl.semaphore_wait(ready, 1)

    def stage_of(t, m, near):
        if t == 0:
            return 1 + (m > 0) * (0 if near else 2)
        return 3 if near else t + 2 + (m > 0)

    def send_down(stage):
        for t in range(n - 1):
            for near in (True, False):
                turns = [m for m in direct
                         if min(stage_of(t, m, near), LAST_STAGE) == stage]
                if turns:
                    @pl.when(t == iz - 1 if near else t < iz - 1)
                    def _():
                        for m in turns:
                            z_copy(iz ^ t, m, aux_hbm.at[0] if stage < 3 else aux.at[0]).start()

    def send_up(first, near, who):
        for t in range(1, n):
            turns = direct[:1] if first else direct[1:]
            if first and near:
                turns = direct
            @pl.when((t == iz + 1 if near else t > iz + 1) & who)
            def _():
                if first:
                    pl.semaphore_wait(z_ready.at[iz ^ t], 1)
                for m in turns:
                    z_copy(iz ^ t, m).start()

    send_down(1)
    for other, me, where, ready in partners:
        @pl.when(other < me)
        def _():
            signal(ready, where)

    with jax.named_scope("latent"):
        load_u.wait()
        total = jnp.zeros(lat_own.shape, F32)
        for j in range(pairs_j):
            pltpu.make_async_copy(d_hbm.at[0, j], d.at[j], d_sem.at[j]).wait()
            if j == 0:
                send_down(2)
            total += jnp.dot(d[j], u[j], preferred_element_type=F32)
        lat_own[...] = total
        plat[...] = total.astype(BF16)

    load_aux.wait()
    send_down(3)
    send_up(True, True, iz > 0)

    def halfway(k, place, pairs):
        for j in pairs:
            block = lax.dot_general(d[j], aux[k], NT, preferred_element_type=F32)
            half[place * width:(place + 1) * width,
                 j * width:(j + 1) * width] = block.astype(BF16)

    def ladder(k, pairs, add):
        cols = slice(pairs[0] * width, (pairs[-1] + 1) * width)
        res = jnp.dot(aux[k], half[:width, cols], preferred_element_type=F32)
        acc[:, cols] = acc[:, cols] + res if add else res

    every = list(range(pairs_j))
    early, late = every[:(pairs_j + 1) // 2], every[(pairs_j + 1) // 2:] or every[-1:]

    def finish(ks):
        left = jnp.concatenate([aux[k] for k in ks] + [lat[...]], axis=1)
        res = jnp.dot(left, half[(2 - len(ks)) * width:, :], preferred_element_type=F32)
        if n > 1:
            res += acc[...]
        for j in range(pairs_j):
            out[0, j] = res[:, j * width:(j + 1) * width].astype(BF16)

    for j in range(pairs_j):
        half[2 * width:, j * width:(j + 1) * width] = u[j].T

    @pl.when(iz >= 0)
    def _():
        halfway(0, 0 if n > 1 else 1, every)
    send_down(4)
    send_up(True, True, iz == 0)
    send_up(True, False, iz > 0)
    for index in range(n - 1, len(partners)):
        await_ready(index)
    p_copy(0).start()
    @pl.when(iz >= 0)
    def _():
        if n > 1:
            ladder(0, every, False)
    send_down(5)
    with jax.named_scope("up"):
        send_up(True, False, iz == 0)

    def pass_on(i):
        k = order[i]
        with jax.named_scope("pass%d" % i):
            z_copy(k, 0).wait_recv()
            for m in relayed:
                r_copy(k, m).start()
            s_copy(k, 0, ij).start()

    def share(i):
        k = order[i]
        with jax.named_scope("shareA%d" % i):
            for m in direct[1:]:
                z_copy(k, m).wait_recv()
                s_copy(k, m, ij).start()
        with jax.named_scope("shareB%d" % i):
            for m in relayed:
                r_copy(k, m, m).wait_recv()
                s_copy(k, m, ij).start()

    def complete(i):
        k = order[i]
        with jax.named_scope("compl%d" % i):
            sent(k, len(spots), s_recv).wait()

    def chip_latent():
        p_copy(0).wait_recv()
        lat_own[...] += lat_sib[...].astype(F32)
        p_copy(0).wait_send()
        plat[...] = lat_own[...].astype(BF16)

    def cross_latent():
        for x in range(1, nx):
            p_copy(x).start()

    def whole_latent():
        with jax.named_scope("wholelat"):
            mine = lat_own[lat_half(core), :]
            for x in range(1, nx):
                p_copy(x).wait_recv()
                mine += lat_in[x].astype(F32)
            lat[lat_half(core), :] = mine.astype(BF16)

    chip_latent()
    for i in range(1, min(2, n)):
        pass_on(i)
    send_up(False, False, iz >= 0)
    for i in range(2, min(4, n)):
        pass_on(i)
    cross_latent()
    for i in range(1, min(2, n)):
        share(i)
    last = list(range(max(n - 2, min(n - 1, 1)), n))
    for i in range(1, last[0]):
        complete(i)
        @pl.when(iz >= 0)
        def _():
            halfway(order[i], 0, early)
        share(i + 1)
        @pl.when(iz >= 0)
        def _():
            halfway(order[i], 0, late)
        if i + 3 < n:
            pass_on(i + 3)
        @pl.when(iz >= 0)
        def _():
            ladder(order[i], early, True)
        if i == last[0] - 1 and len(last) > 1:
            share(last[1])
        @pl.when(iz >= 0)
        def _():
            ladder(order[i], late, True)
    whole_latent()
    l_copy(core).start()
    if last[0] == 1 and len(last) > 1:
        share(last[1])
    for place, i in enumerate(last):
        if i > 0:
            complete(i)
            @pl.when(iz >= 0)
            def _():
                halfway(order[i], 2 - len(last) + place, every)
    l_copy(core ^ 1).wait_recv()
    @pl.when(iz >= 0)
    def _():
        finish([order[i] for i in last])

    with jax.named_scope("tail"):
        for k in range(1, n):
            sent(k, len(direct), z_send).wait()
            if relayed:
                sent(k, len(relayed), r_send).wait()
            sent(k, len(spots), s_send).wait()
        for x in range(1, nx):
            p_copy(x).wait_send()
        l_copy(core).wait_send()


def shards(n, nj, grps, doubles, aux_factors, cycle_factors):
    _, pairs_j, width, _ = doubles.shape
    rank = cycle_factors.shape[2]
    nx = nj // CORES
    ny = grps if width % (grps * nj * 16) == 0 else 1
    others = max(n - 1, 1)
    ahead = 1 + (nx - 1) * (ny - 1)
    dma = pltpu.SemaphoreType.DMA
    flag = pltpu.SemaphoreType.REGULAR
    hbm = pl.BlockSpec(memory_space=pltpu.HBM)
    flops = 4 * n * pairs_j * width**3 + 4 * pairs_j * width * width * rank
    return pl.pallas_call(
        functools.partial(sigma_kernel, n, nj, ny),
        out_shape=pltpu.VMEM(doubles.shape, BF16),
        in_specs=[hbm] * 3,
        out_specs=pl.BlockSpec(memory_space=pltpu.VMEM),
        scratch_shapes=[
            pltpu.VMEM((pairs_j, width, width), BF16),
            pltpu.VMEM((pairs_j, width, rank), BF16),
            pltpu.VMEM((n, width, width), BF16),
            pltpu.VMEM((2 * width + rank, pairs_j * width), BF16),
            pltpu.VMEM((width, pairs_j * width), F32),
            pltpu.VMEM((width, rank), BF16),
            pltpu.VMEM((width, rank), F32),
            pltpu.VMEM((width, rank), BF16),
            pltpu.VMEM((nx, width // CORES, rank), BF16),
            pltpu.VMEM((width, rank), BF16),
            dma((2,)), dma((pairs_j,)),
            flag((n,)), flag((nx,)), flag((ny,)), flag,
            dma((others,)), dma((others * ahead,)),
            dma((others,)), dma((others * max(nx * ny - ahead, 1),)),
            dma((others,)), dma((others,)),
            dma((nx,)), dma((nx,)),
            dma, dma,
        ],
        compiler_params=pltpu.CompilerParams(
            collective_id=0, has_side_effects=True, vmem_limit_bytes=67043328 - doubles.size * 2 - 2**16),
        cost_estimate=pl.CostEstimate(
            flops=flops, bytes_accessed=4 * doubles.size, transcendentals=0),
    )(doubles, aux_factors, cycle_factors)


def solution(mesh):
    in_specs = (P(("grp", "ia"), "ja", None, None), P("ia", None, None), P())
    out_specs = P(("grp", "ia"), "ja", None, None)
    body = functools.partial(shards, mesh.shape["ia"], mesh.shape["ja"], mesh.shape["grp"])
    return jax.shard_map(body, mesh=mesh, in_specs=in_specs, out_specs=out_specs, check_vma=False)
```

```python
import functools

import jax
import jax.numpy as jnp
from jax import lax
from jax.experimental import pallas as pl
from jax.experimental.pallas import tpu as pltpu
from jax.sharding import PartitionSpec as P

MESH = pl.DeviceIdType.MESH
F32 = jnp.float32
BF16 = jnp.bfloat16
NT = (((1,), (1,)), ((), ()))
CORES = 2
LAST_STAGE = 5
NEAR_SECOND, FAR_SECOND, MID_FIRST, MID_SECOND, LAG = 3, 3, 2, 3, 1
SPLIT = 1


def sigma_kernel(n, nj, ny, d_hbm, aux_hbm, u_hbm, out, d, u, aux, half, acc,
                 plat, lat_own, lat_sib, lat_in, lat, load_sem, d_sem,
                 z_ready, x_ready, y_ready, s_ready, sends, prime_recv, late_recv, s_recv,
                 p_send, p_recv, l_send, l_recv):
    nx = nj // CORES
    pairs_j, width, _ = d.shape
    rows = width // (ny * nj)
    lat_rows = width // CORES
    iz = lax.axis_index("ia")
    iy = lax.axis_index("grp") if ny > 1 else 0
    ij = lax.axis_index("ja")
    core = ij % CORES
    sibling = {"ja": ij ^ 1}
    spots = [(y, x) for y in range(ny) for x in range(nx)]
    direct = [0] + [m for m, (y, x) in enumerate(spots) if y > 0 and x > 0]
    relayed = [m for m in range(1, len(spots)) if m not in direct]

    def piece(m, base):
        y, x = spots[m]
        owner = (iy ^ y) * nj + (base ^ (CORES * x))
        return pl.ds(pl.multiple_of(owner * rows, rows), rows)

    def lat_half(c):
        return pl.ds(pl.multiple_of(c * lat_rows, lat_rows), lat_rows)

    def plane(m):
        y, x = spots[m]
        return {"grp": iy ^ y} if x == 0 else {"ja": ij ^ (CORES * x)}

    load_aux = pltpu.make_async_copy(aux_hbm.at[0], aux.at[0], load_sem.at[0])
    load_u = pltpu.make_async_copy(
        u_hbm.at[pl.ds(ij * pairs_j, pairs_j)], u, load_sem.at[1])

    def load_d(j, part):
        share_of = pl.ds(part * (width // SPLIT), width // SPLIT)
        return pltpu.make_async_copy(d_hbm.at[0, j, share_of], d.at[j, share_of],
                                     d_sem.at[j])

    orders = [sorted(range(1, n), key=lambda k: (abs((z ^ k) - z) if z ^ k < z else n, k)) for z in range(n)]
    order = [0] + [sum(jnp.where(iz == z, orders[z][i], 0) for z in range(n))
                   for i in range(n - 1)]

    load_u.start()
    for j in range(pairs_j):
        for part in range(SPLIT):
            load_d(j, part).start()
    load_aux.start()

    def remote(src, dst, send, recv, where):
        return pltpu.make_async_remote_copy(
            src_ref=src, dst_ref=dst, send_sem=send, recv_sem=recv,
            device_id=where, device_id_type=MESH)

    def z_copy(k, m, src=aux.at[0]):
        return remote(src.at[piece(m, ij)], aux.at[k, piece(m, ij)],
                      sends.at[k - 1], (late_recv if m > 0 else prime_recv).at[k - 1],
                      {"ia": iz ^ k})

    def r_copy(k, m, from_m=0):
        part = aux.at[k, piece(from_m, ij)]
        return remote(part, part, sends.at[k - 1], late_recv.at[k - 1], plane(m))

    def s_copy(k, m, base):
        part = aux.at[k, piece(m, base)]
        return remote(part, part, sends.at[k - 1], s_recv.at[k - 1], sibling)

    def sent(k, count, sem):
        part = aux.at[k, pl.ds(0, count * rows)]
        return pltpu.make_async_copy(part, part, sem.at[k - 1])

    def p_copy(x):
        if x == 0:
            return remote(plat, lat_sib, p_send.at[0], p_recv.at[0], sibling)
        return remote(plat.at[lat_half(core)], lat_in.at[x], p_send.at[x], p_recv.at[x],
                      {"ja": ij ^ (CORES * x)})

    def l_copy(c):
        return remote(lat.at[lat_half(c)], lat.at[lat_half(c)], l_send, l_recv, sibling)

    def signal(sem, where):
        pl.semaphore_signal(sem, inc=1, device_id=where, device_id_type=MESH)

    partners = [(iz ^ k, iz, {"ia": iz ^ k}, z_ready.at[k - 1]) for k in range(1, n)]
    partners += [(ij ^ (CORES * x), ij, {"ja": ij ^ (CORES * x)}, x_ready.at[x - 1])
                 for x in range(1, nx)]
    partners += [(ij ^ 1, ij, sibling, s_ready)]
    partners += [(iy ^ y, iy, {"grp": iy ^ y}, y_ready.at[y - 1]) for y in range(1, ny)]

    barrier = pltpu.get_barrier_semaphore()
    for other, me, where, _ in partners:
        @pl.when(other > me)
        def _():
            signal(barrier, where)
    lower = iz + ij // CORES + core + iy

    @pl.when(lower > 0)
    def _():
        pl.semaphore_wait(barrier, lower)

    def await_ready(index):
        other, me, _, ready = partners[index]

        @pl.when(other > me)
        def _():
            pl.semaphore_wait(ready, 1)

    def stage_of(t, m, near):
        if t == 0:
            return (NEAR_SECOND if near else FAR_SECOND) if m > 0 else 1
        if near:
            return MID_SECOND if m > 0 else MID_FIRST
        return t + 2 + LAG * (m > 0)

    def send_down(stage):
        for t in range(n - 1):
            for near in (True, False):
                turns = [m for m in direct
                         if min(stage_of(t, m, near), LAST_STAGE) == stage]
                if turns:
                    @pl.when(t == iz - 1 if near else t < iz - 1)
                    def _():
                        for m in turns:
                            z_copy(iz ^ t, m, aux_hbm.at[0] if stage < 3 else aux.at[0]).start()

    def send_up(first, near, who):
        for t in range(1, n):
            turns = direct[:1] if first else direct[1:]
            if first and near:
                turns = direct
            @pl.when((t == iz + 1 if near else t > iz + 1) & who)
            def _():
                if first:
                    pl.semaphore_wait(z_ready.at[(iz ^ t) - 1], 1)
                for m in turns:
                    z_copy(iz ^ t, m).start()

    send_down(1)
    for other, me, where, ready in partners:
        @pl.when(other < me)
        def _():
            signal(ready, where)

    with jax.named_scope("latent"):
        load_u.wait()
        total = jnp.zeros(lat_own.shape, F32)
        for j in range(pairs_j):
            pltpu.make_async_copy(d_hbm.at[0, j], d.at[j], d_sem.at[j]).wait()
            if j == 0:
                send_down(2)
            total += jnp.dot(d[j], u[j], preferred_element_type=F32)
        lat_own[...] = total
        plat[...] = total.astype(BF16)

    load_aux.wait()
    send_down(3)
    send_up(True, True, iz > 0)

    def halfway(k, place, pairs):
        for j in pairs:
            block = lax.dot_general(d[j], aux[k], NT, preferred_element_type=F32)
            half[place * width:(place + 1) * width,
                 j * width:(j + 1) * width] = block.astype(BF16)

    def ladder(k, pairs, add):
        cols = slice(pairs[0] * width, (pairs[-1] + 1) * width)
        res = jnp.dot(aux[k], half[:width, cols], preferred_element_type=F32)
        acc[:, cols] = acc[:, cols] + res if add else res

    every = list(range(pairs_j))
    early, late = every[:(pairs_j + 1) // 2], every[(pairs_j + 1) // 2:] or every[-1:]

    def finish(ks):
        left = jnp.concatenate([aux[k] for k in ks] + [lat[...]], axis=1)
        res = jnp.dot(left, half[(2 - len(ks)) * width:, :], preferred_element_type=F32)
        if n > 1:
            res += acc[...]
        for j in range(pairs_j):
            out[0, j] = res[:, j * width:(j + 1) * width].astype(BF16)

    def pass_on(i):
        k = order[i]
        with jax.named_scope("pass%d" % i):
            z_copy(k, 0).wait_recv()
            for m in relayed:
                r_copy(k, m).start()
            s_copy(k, 0, ij).start()

    for j in range(pairs_j):
        half[2 * width:, j * width:(j + 1) * width] = u[j].T

    @pl.when(iz >= 0)
    def _():
        halfway(0, 0 if n > 1 else 1, every)
    send_down(4)
    send_up(True, True, iz == 0)
    send_up(True, False, iz > 0)
    for index in range(n - 1, len(partners)):
        await_ready(index)
    p_copy(0).start()
    if n > 1:
        @pl.when(iz == 0)
        def _():
            pass_on(1)

    @pl.when(iz >= 0)
    def _():
        if n > 1:
            ladder(0, every, False)
    send_down(5)
    with jax.named_scope("up"):
        send_up(True, False, iz == 0)

    def share(i):
        k = order[i]
        with jax.named_scope("share%d" % i):
            if len(spots) > 1:
                sent(k, len(spots) - 1, late_recv).wait()
            for m in direct[1:] + relayed:
                s_copy(k, m, ij).start()

    def complete(i):
        k = order[i]
        with jax.named_scope("compl%d" % i):
            sent(k, len(spots), s_recv).wait()

    def chip_latent():
        p_copy(0).wait_recv()
        lat_own[...] += lat_sib[...].astype(F32)
        p_copy(0).wait_send()
        plat[...] = lat_own[...].astype(BF16)

    def cross_latent():
        for x in range(1, nx):
            p_copy(x).start()

    def whole_latent():
        with jax.named_scope("wholelat"):
            mine = lat_own[lat_half(core), :]
            for x in range(1, nx):
                p_copy(x).wait_recv()
                mine += lat_in[x].astype(F32)
            lat[lat_half(core), :] = mine.astype(BF16)

    chip_latent()
    if n > 1:
        @pl.when(iz > 0)
        def _():
            pass_on(1)

    send_up(False, False, iz >= 0)
    for i in range(2, min(4, n)):
        pass_on(i)
    cross_latent()
    for i in range(1, min(2, n)):
        share(i)
    last = list(range(max(n - 2, min(n - 1, 1)), n))
    for i in range(1, last[0]):
        complete(i)
        @pl.when(iz >= 0)
        def _():
            halfway(order[i], 0, early)

        @pl.when(iz == 0)
        def _():
            share(i + 1)

        @pl.when(iz >= 0)
        def _():
            halfway(order[i], 0, late)
        if i + 3 < n:
            pass_on(i + 3)
        @pl.when(iz >= 0)
        def _():
            ladder(order[i], early, True)

        @pl.when(iz > 0)
        def _():
            share(i + 1)

        if i == last[0] - 1 and len(last) > 1:
            share(last[1])
        @pl.when(iz >= 0)
        def _():
            ladder(order[i], late, True)
    whole_latent()
    l_copy(core).start()
    if last[0] == 1 and len(last) > 1:
        share(last[1])
    for place, i in enumerate(last):
        if i > 0:
            complete(i)
            @pl.when(iz >= 0)
            def _():
                halfway(order[i], 2 - len(last) + place, every)
    l_copy(core ^ 1).wait_recv()
    @pl.when(iz >= 0)
    def _():
        finish([order[i] for i in last])

    with jax.named_scope("tail"):
        for k in range(1, n):
            sent(k, 2 * len(spots), sends).wait()
        for x in range(1, nx):
            p_copy(x).wait_send()
        l_copy(core).wait_send()


def shards(n, nj, grps, doubles, aux_factors, cycle_factors):
    _, pairs_j, width, _ = doubles.shape
    rank = cycle_factors.shape[2]
    nx = nj // CORES
    ny = grps if width % (grps * nj * 16) == 0 else 1
    others = max(n - 1, 1)
    dma = pltpu.SemaphoreType.DMA
    flag = pltpu.SemaphoreType.REGULAR
    hbm = pl.BlockSpec(memory_space=pltpu.HBM)
    flops = 4 * n * pairs_j * width**3 + 4 * pairs_j * width * width * rank
    return pl.pallas_call(
        functools.partial(sigma_kernel, n, nj, ny),
        out_shape=pltpu.VMEM(doubles.shape, BF16),
        in_specs=[hbm] * 3,
        out_specs=pl.BlockSpec(memory_space=pltpu.VMEM),
        scratch_shapes=[
            pltpu.VMEM((pairs_j, width, width), BF16),
            pltpu.VMEM((pairs_j, width, rank), BF16),
            pltpu.VMEM((n, width, width), BF16),
            pltpu.VMEM((2 * width + rank, pairs_j * width), BF16),
            pltpu.VMEM((width, pairs_j * width), F32),
            pltpu.VMEM((width, rank), BF16),
            pltpu.VMEM((width, rank), F32),
            pltpu.VMEM((width, rank), BF16),
            pltpu.VMEM((nx, width // CORES, rank), BF16),
            pltpu.VMEM((width, rank), BF16),
            dma((2,)), dma((pairs_j,)),
            flag((others,)), flag((max(nx - 1, 1),)), flag((max(ny - 1, 1),)), flag,
            dma((others,)), dma((others,)), dma((others,)), dma((others,)),
            dma((nx,)), dma((nx,)),
            dma, dma,
        ],
        compiler_params=pltpu.CompilerParams(
            collective_id=0, has_side_effects=True, vmem_limit_bytes=67043328 - doubles.size * 2 - 2**16),
        cost_estimate=pl.CostEstimate(
            flops=flops, bytes_accessed=4 * doubles.size, transcendentals=0),
    )(doubles, aux_factors, cycle_factors)


def solution(mesh):
    in_specs = (P(("grp", "ia"), "ja", None, None), P("ia", None, None), P())
    out_specs = P(("grp", "ia"), "ja", None, None)
    body = functools.partial(shards, mesh.shape["ia"], mesh.shape["ja"], mesh.shape["grp"])
    return jax.shard_map(body, mesh=mesh, in_specs=in_specs, out_specs=out_specs, check_vma=False)
```

```python
import functools

import jax
import jax.numpy as jnp
from jax import lax
from jax.experimental import pallas as pl
from jax.experimental.pallas import tpu as pltpu
from jax.sharding import PartitionSpec as P

MESH = pl.DeviceIdType.MESH
F32 = jnp.float32
BF16 = jnp.bfloat16
NT = (((1,), (1,)), ((), ()))
CORES = 2
LAST_STAGE = 5
NEAR_SECOND, FAR_SECOND, MID_FIRST, MID_SECOND, LAG = 3, 3, 2, 3, 1
SPLIT = 1


def sigma_kernel(n, nj, ny, d_hbm, aux_hbm, u_hbm, out, d, u, aux, half, acc,
                 plat, lat_own, lat_sib, lat_in, lat, load_sem, d_sem,
                 z_ready, x_ready, y_ready, s_ready, sends, prime_recv, late_recv, s_recv,
                 p_send, p_recv, l_send, l_recv):
    nx = nj // CORES
    pairs_j, width, _ = d.shape
    rows = width // (ny * nj)
    lat_rows = width // CORES
    iz = lax.axis_index("ia")
    iy = lax.axis_index("grp") if ny > 1 else 0
    ij = lax.axis_index("ja")
    core = ij % CORES
    sibling = {"ja": ij ^ 1}
    spots = [(y, x) for y in range(ny) for x in range(nx)]
    direct = [0] + [m for m, (y, x) in enumerate(spots) if y > 0 and x > 0]
    relayed = [m for m in range(1, len(spots)) if m not in direct]

    def piece(m, base):
        y, x = spots[m]
        owner = (iy ^ y) * nj + (base ^ (CORES * x))
        return pl.ds(pl.multiple_of(owner * rows, rows), rows)

    def lat_half(c):
        return pl.ds(pl.multiple_of(c * lat_rows, lat_rows), lat_rows)

    def plane(m):
        y, x = spots[m]
        return {"grp": iy ^ y} if x == 0 else {"ja": ij ^ (CORES * x)}

    load_aux = pltpu.make_async_copy(aux_hbm.at[0], aux.at[0], load_sem.at[0])
    load_u = pltpu.make_async_copy(
        u_hbm.at[pl.ds(ij * pairs_j, pairs_j)], u, load_sem.at[1])

    def load_d(j, part):
        share_of = pl.ds(part * (width // SPLIT), width // SPLIT)
        return pltpu.make_async_copy(d_hbm.at[0, j, share_of], d.at[j, share_of],
                                     d_sem.at[j])

    orders = [sorted(range(1, n), key=lambda k: (abs((z ^ k) - z) if z ^ k < z else n, k)) for z in range(n)]
    order = [0] + [sum(jnp.where(iz == z, orders[z][i], 0) for z in range(n))
                   for i in range(n - 1)]

    load_u.start()
    for j in range(pairs_j):
        for part in range(SPLIT):
            load_d(j, part).start()
    load_aux.start()

    def remote(src, dst, send, recv, where):
        return pltpu.make_async_remote_copy(
            src_ref=src, dst_ref=dst, send_sem=send, recv_sem=recv,
            device_id=where, device_id_type=MESH)

    def z_copy(k, m, src=aux.at[0]):
        return remote(src.at[piece(m, ij)], aux.at[k, piece(m, ij)],
                      sends.at[k - 1], (late_recv if m > 0 else prime_recv).at[k - 1],
                      {"ia": iz ^ k})

    def r_copy(k, m, from_m=0):
        part = aux.at[k, piece(from_m, ij)]
        return remote(part, part, sends.at[k - 1], late_recv.at[k - 1], plane(m))

    def s_copy(k, m, base):
        part = aux.at[k, piece(m, base)]
        return remote(part, part, sends.at[k - 1], s_recv.at[k - 1], sibling)

    def sent(k, count, sem):
        part = aux.at[k, pl.ds(0, count * rows)]
        return pltpu.make_async_copy(part, part, sem.at[k - 1])

    def p_copy(x):
        if x == 0:
            return remote(plat, lat_sib, p_send.at[0], p_recv.at[0], sibling)
        return remote(plat.at[lat_half(core)], lat_in.at[x], p_send.at[x], p_recv.at[x],
                      {"ja": ij ^ (CORES * x)})

    def l_copy(c):
        return remote(lat.at[lat_half(c)], lat.at[lat_half(c)], l_send, l_recv, sibling)

    def signal(sem, where):
        pl.semaphore_signal(sem, inc=1, device_id=where, device_id_type=MESH)

    partners = [(iz ^ k, iz, {"ia": iz ^ k}, z_ready.at[k - 1]) for k in range(1, n)]
    partners += [(ij ^ (CORES * x), ij, {"ja": ij ^ (CORES * x)}, x_ready.at[x - 1])
                 for x in range(1, nx)]
    partners += [(ij ^ 1, ij, sibling, s_ready)]
    partners += [(iy ^ y, iy, {"grp": iy ^ y}, y_ready.at[y - 1]) for y in range(1, ny)]

    barrier = pltpu.get_barrier_semaphore()
    for other, me, where, _ in partners:
        @pl.when(other > me)
        def _():
            signal(barrier, where)
    lower = iz + ij // CORES + core + iy

    @pl.when(lower > 0)
    def _():
        pl.semaphore_wait(barrier, lower)

    def await_ready(index):
        other, me, _, ready = partners[index]

        @pl.when(other > me)
        def _():
            pl.semaphore_wait(ready, 1)

    def stage_of(t, m, near):
        if t == 0:
            return (NEAR_SECOND if near else FAR_SECOND) if m > 0 else 1
        if near:
            return MID_SECOND if m > 0 else MID_FIRST
        return t + 2 + LAG * (m > 0)

    def send_down(stage):
        for t in range(n - 1):
            for near in (True, False):
                turns = [m for m in direct
                         if min(stage_of(t, m, near), LAST_STAGE) == stage]
                if turns:
                    @pl.when(t == iz - 1 if near else t < iz - 1)
                    def _():
                        for m in turns:
                            z_copy(iz ^ t, m, aux_hbm.at[0] if stage < 3 else aux.at[0]).start()

    def send_up(first, near, who):
        for t in range(1, n):
            turns = direct[:1] if first else direct[1:]
            if first and near:
                turns = direct
            @pl.when((t == iz + 1 if near else t > iz + 1) & who)
            def _():
                if first:
                    pl.semaphore_wait(z_ready.at[(iz ^ t) - 1], 1)
                for m in turns:
                    z_copy(iz ^ t, m).start()

    send_down(1)
    for other, me, where, ready in partners:
        @pl.when(other < me)
        def _():
            signal(ready, where)

    with jax.named_scope("latent"):
        load_u.wait()
        total = jnp.zeros(lat_own.shape, F32)
        for j in range(pairs_j):
            pltpu.make_async_copy(d_hbm.at[0, j], d.at[j], d_sem.at[j]).wait()
            if j == 0:
                send_down(2)
            total += jnp.dot(d[j], u[j], preferred_element_type=F32)
        lat_own[...] = total
        plat[...] = total.astype(BF16)

    load_aux.wait()
    send_down(3)
    send_up(True, True, iz > 0)
    sibling_index = n - 1 + nx - 1
    await_ready(sibling_index)
    p_copy(0).start()

    def chip_latent():
        p_copy(0).wait_recv()
        lat_own[...] += lat_sib[...].astype(F32)
        p_copy(0).wait_send()
        plat[...] = lat_own[...].astype(BF16)

    def cross_latent():
        for x in range(1, nx):
            p_copy(x).start()

    def halfway(k, place, pairs):
        for j in pairs:
            block = lax.dot_general(d[j], aux[k], NT, preferred_element_type=F32)
            half[place * width:(place + 1) * width,
                 j * width:(j + 1) * width] = block.astype(BF16)

    def ladder(k, pairs, add):
        cols = slice(pairs[0] * width, (pairs[-1] + 1) * width)
        res = jnp.dot(aux[k], half[:width, cols], preferred_element_type=F32)
        acc[:, cols] = acc[:, cols] + res if add else res

    every = list(range(pairs_j))
    early, late = every[:(pairs_j + 1) // 2], every[(pairs_j + 1) // 2:] or every[-1:]

    def finish(ks):
        left = jnp.concatenate([aux[k] for k in ks] + [lat[...]], axis=1)
        res = jnp.dot(left, half[(2 - len(ks)) * width:, :], preferred_element_type=F32)
        if n > 1:
            res += acc[...]
        for j in range(pairs_j):
            out[0, j] = res[:, j * width:(j + 1) * width].astype(BF16)

    def pass_on(i):
        k = order[i]
        with jax.named_scope("pass%d" % i):
            z_copy(k, 0).wait_recv()
            for m in relayed:
                r_copy(k, m).start()
            s_copy(k, 0, ij).start()

    for j in range(pairs_j):
        half[2 * width:, j * width:(j + 1) * width] = u[j].T

    @pl.when(iz >= 0)
    def _():
        halfway(0, 0 if n > 1 else 1, every)
    send_down(4)
    send_up(True, True, iz == 0)
    send_up(True, False, iz > 0)
    for index in range(n - 1, len(partners)):
        if index != sibling_index:
            await_ready(index)
    chip_latent()
    if n > 1:
        @pl.when(iz == 0)
        def _():
            pass_on(1)

    @pl.when(iz >= 0)
    def _():
        if n > 1:
            ladder(0, every, False)
    cross_latent()
    send_down(5)
    with jax.named_scope("up"):
        send_up(True, False, iz == 0)

    def share(i):
        k = order[i]
        with jax.named_scope("share%d" % i):
            if len(spots) > 1:
                sent(k, len(spots) - 1, late_recv).wait()
            for m in direct[1:] + relayed:
                s_copy(k, m, ij).start()

    def complete(i):
        k = order[i]
        with jax.named_scope("compl%d" % i):
            sent(k, len(spots), s_recv).wait()

    def whole_latent():
        with jax.named_scope("wholelat"):
            mine = lat_own[lat_half(core), :]
            for x in range(1, nx):
                p_copy(x).wait_recv()
                mine += lat_in[x].astype(F32)
            lat[lat_half(core), :] = mine.astype(BF16)

    if n > 1:
        @pl.when(iz > 0)
        def _():
            pass_on(1)

    send_up(False, False, iz >= 0)
    for i in range(2, min(4, n)):
        pass_on(i)
    for i in range(1, min(2, n)):
        share(i)
    last = list(range(max(n - 2, min(n - 1, 1)), n))
    for i in range(1, last[0]):
        complete(i)
        @pl.when(iz >= 0)
        def _():
            halfway(order[i], 0, early)

        @pl.when(iz >= 0)
        def _():
            halfway(order[i], 0, late)
        if i + 3 < n:
            pass_on(i + 3)
        @pl.when(iz >= 0)
        def _():
            ladder(order[i], early, True)

        share(i + 1)
        if i == last[0] - 1 and len(last) > 1:
            share(last[1])
        @pl.when(iz >= 0)
        def _():
            ladder(order[i], late, True)
    whole_latent()
    l_copy(core).start()
    if last[0] == 1 and len(last) > 1:
        share(last[1])
    for place, i in enumerate(last):
        if i > 0:
            complete(i)
            @pl.when(iz >= 0)
            def _():
                halfway(order[i], 2 - len(last) + place, every)
    l_copy(core ^ 1).wait_recv()
    @pl.when(iz >= 0)
    def _():
        finish([order[i] for i in last])

    with jax.named_scope("tail"):
        for k in range(1, n):
            sent(k, 2 * len(spots), sends).wait()
        for x in range(1, nx):
            p_copy(x).wait_send()
        l_copy(core).wait_send()


def shards(n, nj, grps, doubles, aux_factors, cycle_factors):
    _, pairs_j, width, _ = doubles.shape
    rank = cycle_factors.shape[2]
    nx = nj // CORES
    ny = grps if width % (grps * nj * 16) == 0 else 1
    others = max(n - 1, 1)
    dma = pltpu.SemaphoreType.DMA
    flag = pltpu.SemaphoreType.REGULAR
    hbm = pl.BlockSpec(memory_space=pltpu.HBM)
    flops = 4 * n * pairs_j * width**3 + 4 * pairs_j * width * width * rank
    return pl.pallas_call(
        functools.partial(sigma_kernel, n, nj, ny),
        out_shape=pltpu.VMEM(doubles.shape, BF16),
        in_specs=[hbm] * 3,
        out_specs=pl.BlockSpec(memory_space=pltpu.VMEM),
        scratch_shapes=[
            pltpu.VMEM((pairs_j, width, width), BF16),
            pltpu.VMEM((pairs_j, width, rank), BF16),
            pltpu.VMEM((n, width, width), BF16),
            pltpu.VMEM((2 * width + rank, pairs_j * width), BF16),
            pltpu.VMEM((width, pairs_j * width), F32),
            pltpu.VMEM((width, rank), BF16),
            pltpu.VMEM((width, rank), F32),
            pltpu.VMEM((width, rank), BF16),
            pltpu.VMEM((nx, width // CORES, rank), BF16),
            pltpu.VMEM((width, rank), BF16),
            dma((2,)), dma((pairs_j,)),
            flag((others,)), flag((max(nx - 1, 1),)), flag((max(ny - 1, 1),)), flag,
            dma((others,)), dma((others,)), dma((others,)), dma((others,)),
            dma((nx,)), dma((nx,)),
            dma, dma,
        ],
        compiler_params=pltpu.CompilerParams(
            collective_id=0, has_side_effects=True, vmem_limit_bytes=67043328 - doubles.size * 2 - 2**16),
        cost_estimate=pl.CostEstimate(
            flops=flops, bytes_accessed=4 * doubles.size, transcendentals=0),
    )(doubles, aux_factors, cycle_factors)


def solution(mesh):
    in_specs = (P(("grp", "ia"), "ja", None, None), P("ia", None, None), P())
    out_specs = P(("grp", "ia"), "ja", None, None)
    body = functools.partial(shards, mesh.shape["ia"], mesh.shape["ja"], mesh.shape["grp"])
    return jax.shard_map(body, mesh=mesh, in_specs=in_specs, out_specs=out_specs, check_vma=False)
```

```python
import functools

import jax
import jax.numpy as jnp
from jax import lax
from jax.experimental import pallas as pl
from jax.experimental.pallas import tpu as pltpu
from jax.sharding import PartitionSpec as P

MESH = pl.DeviceIdType.MESH
F32 = jnp.float32
BF16 = jnp.bfloat16
NT = (((1,), (1,)), ((), ()))
CORES = 2
LAST_STAGE = 5
NEAR_SECOND, FAR_SECOND, MID_FIRST, MID_SECOND, LAG = 3, 3, 2, 3, 1
SPLIT = 1


def sigma_kernel(n, nj, ny, d_hbm, aux_hbm, u_hbm, out, d, u, aux, half, acc,
                 plat, lat_own, lat_sib, lat_in, lat, load_sem, d_sem,
                 z_ready, x_ready, y_ready, s_ready, sends, prime_recv, late_recv, s_recv,
                 p_send, p_recv, l_send, l_recv):
    nx = nj // CORES
    pairs_j, width, _ = d.shape
    rows = width // (ny * nj)
    lat_rows = width // CORES
    iz = lax.axis_index("ia")
    iy = lax.axis_index("grp") if ny > 1 else 0
    ij = lax.axis_index("ja")
    core = ij % CORES
    sibling = {"ja": ij ^ 1}
    spots = [(y, x) for y in range(ny) for x in range(nx)]
    direct = [0] + [m for m, (y, x) in enumerate(spots) if y > 0 and x > 0]
    relayed = [m for m in range(1, len(spots)) if m not in direct]

    def piece(m, base):
        y, x = spots[m]
        owner = (iy ^ y) * nj + (base ^ (CORES * x))
        return pl.ds(pl.multiple_of(owner * rows, rows), rows)

    def lat_half(c):
        return pl.ds(pl.multiple_of(c * lat_rows, lat_rows), lat_rows)

    def plane(m):
        y, x = spots[m]
        return {"grp": iy ^ y} if x == 0 else {"ja": ij ^ (CORES * x)}

    load_aux = pltpu.make_async_copy(aux_hbm.at[0], aux.at[0], load_sem.at[0])
    load_u = pltpu.make_async_copy(
        u_hbm.at[pl.ds(ij * pairs_j, pairs_j)], u, load_sem.at[1])

    def load_d(j, part):
        share_of = pl.ds(part * (width // SPLIT), width // SPLIT)
        return pltpu.make_async_copy(d_hbm.at[0, j, share_of], d.at[j, share_of],
                                     d_sem.at[j])

    orders = [sorted(range(1, n), key=lambda k: (abs((z ^ k) - z) if z ^ k < z else n, k)) for z in range(n)]
    order = [0] + [sum(jnp.where(iz == z, orders[z][i], 0) for z in range(n))
                   for i in range(n - 1)]

    load_u.start()
    for j in range(pairs_j):
        for part in range(SPLIT):
            load_d(j, part).start()
    load_aux.start()

    def remote(src, dst, send, recv, where):
        return pltpu.make_async_remote_copy(
            src_ref=src, dst_ref=dst, send_sem=send, recv_sem=recv,
            device_id=where, device_id_type=MESH)

    def z_copy(k, m, src=aux.at[0]):
        return remote(src.at[piece(m, ij)], aux.at[k, piece(m, ij)],
                      sends.at[k - 1], (late_recv if m > 0 else prime_recv).at[k - 1],
                      {"ia": iz ^ k})

    def r_copy(k, m, from_m=0):
        part = aux.at[k, piece(from_m, ij)]
        return remote(part, part, sends.at[k - 1], late_recv.at[k - 1], plane(m))

    def s_copy(k, m, base):
        part = aux.at[k, piece(m, base)]
        return remote(part, part, sends.at[k - 1], s_recv.at[k - 1], sibling)

    def sent(k, count, sem):
        part = aux.at[k, pl.ds(0, count * rows)]
        return pltpu.make_async_copy(part, part, sem.at[k - 1])

    def p_copy(x):
        if x == 0:
            return remote(plat, lat_sib, p_send.at[0], p_recv.at[0], sibling)
        return remote(plat.at[lat_half(core)], lat_in.at[x], p_send.at[x], p_recv.at[x],
                      {"ja": ij ^ (CORES * x)})

    def l_copy(c):
        return remote(lat.at[lat_half(c)], lat.at[lat_half(c)], l_send, l_recv, sibling)

    def signal(sem, where):
        pl.semaphore_signal(sem, inc=1, device_id=where, device_id_type=MESH)

    partners = [(iz ^ k, iz, {"ia": iz ^ k}, z_ready.at[k - 1]) for k in range(1, n)]
    partners += [(ij ^ (CORES * x), ij, {"ja": ij ^ (CORES * x)}, x_ready.at[x - 1])
                 for x in range(1, nx)]
    partners += [(ij ^ 1, ij, sibling, s_ready)]
    partners += [(iy ^ y, iy, {"grp": iy ^ y}, y_ready.at[y - 1]) for y in range(1, ny)]

    barrier = pltpu.get_barrier_semaphore()
    for other, me, where, _ in partners:
        @pl.when(other > me)
        def _():
            signal(barrier, where)
    lower = iz + ij // CORES + core + iy

    @pl.when(lower > 0)
    def _():
        pl.semaphore_wait(barrier, lower)

    def await_ready(index):
        other, me, _, ready = partners[index]

        @pl.when(other > me)
        def _():
            pl.semaphore_wait(ready, 1)

    def stage_of(t, m, near):
        if t == 0:
            return (NEAR_SECOND if near else FAR_SECOND) if m > 0 else 1
        if near:
            return MID_SECOND if m > 0 else MID_FIRST
        return t + 2 + LAG * (m > 0)

    def send_down(stage):
        for t in range(n - 1):
            for near in (True, False):
                turns = [m for m in direct
                         if min(stage_of(t, m, near), LAST_STAGE) == stage]
                if turns:
                    @pl.when(t == iz - 1 if near else t < iz - 1)
                    def _():
                        for m in turns:
                            z_copy(iz ^ t, m, aux_hbm.at[0] if stage < 3 else aux.at[0]).start()

    def send_up(first, near, who):
        for t in range(1, n):
            turns = direct[:1] if first else direct[1:]
            if first and near:
                turns = direct
            @pl.when((t == iz + 1 if near else t > iz + 1) & who)
            def _():
                if first:
                    pl.semaphore_wait(z_ready.at[(iz ^ t) - 1], 1)
                for m in turns:
                    z_copy(iz ^ t, m).start()

    send_down(1)
    for other, me, where, ready in partners:
        @pl.when(other < me)
        def _():
            signal(ready, where)

    with jax.named_scope("latent"):
        load_u.wait()
        total = jnp.zeros(lat_own.shape, F32)
        for j in range(pairs_j):
            pltpu.make_async_copy(d_hbm.at[0, j], d.at[j], d_sem.at[j]).wait()
            if j == 0:
                send_down(2)
            total += jnp.dot(d[j], u[j], preferred_element_type=F32)
        lat_own[...] = total
        plat[...] = total.astype(BF16)

    load_aux.wait()
    send_down(3)
    send_up(True, True, iz > 0)
    sibling_index = n - 1 + nx - 1
    await_ready(sibling_index)
    p_copy(0).start()

    def chip_latent():
        p_copy(0).wait_recv()
        lat_own[...] += lat_sib[...].astype(F32)
        p_copy(0).wait_send()
        plat[...] = lat_own[...].astype(BF16)

    def cross_latent():
        for x in range(1, nx):
            p_copy(x).start()

    def halfway(k, place, pairs):
        for j in pairs:
            block = lax.dot_general(d[j], aux[k], NT, preferred_element_type=F32)
            half[place * width:(place + 1) * width,
                 j * width:(j + 1) * width] = block.astype(BF16)

    def ladder(k, pairs, add):
        cols = slice(pairs[0] * width, (pairs[-1] + 1) * width)
        res = jnp.dot(aux[k], half[:width, cols], preferred_element_type=F32)
        acc[:, cols] = acc[:, cols] + res if add else res

    every = list(range(pairs_j))
    early, late = every[:(pairs_j + 1) // 2], every[(pairs_j + 1) // 2:] or every[-1:]

    def finish(ks):
        left = jnp.concatenate([aux[k] for k in ks] + [lat[...]], axis=1)
        res = jnp.dot(left, half[(2 - len(ks)) * width:, :], preferred_element_type=F32)
        if n > 1:
            res += acc[...]
        for j in range(pairs_j):
            out[0, j] = res[:, j * width:(j + 1) * width].astype(BF16)

    def pass_on(i):
        k = order[i]
        with jax.named_scope("pass%d" % i):
            z_copy(k, 0).wait_recv()
            for m in relayed:
                r_copy(k, m).start()
            s_copy(k, 0, ij).start()

    for j in range(pairs_j):
        half[2 * width:, j * width:(j + 1) * width] = u[j].T

    @pl.when(iz >= 0)
    def _():
        halfway(0, 0 if n > 1 else 1, every)
    send_down(4)
    send_up(True, True, iz == 0)
    send_up(True, False, iz > 0)
    for index in range(n - 1, len(partners)):
        if index != sibling_index:
            await_ready(index)
    chip_latent()
    if n > 1:
        @pl.when(iz == 0)
        def _():
            pass_on(1)

    @pl.when(iz >= 0)
    def _():
        if n > 1:
            ladder(0, every, False)
    cross_latent()
    send_down(5)
    with jax.named_scope("up"):
        send_up(True, False, iz == 0)

    def share(i):
        k = order[i]
        with jax.named_scope("share%d" % i):
            if len(spots) > 1:
                sent(k, len(spots) - 1, late_recv).wait()
            for m in direct[1:] + relayed:
                s_copy(k, m, ij).start()

    def complete(i):
        k = order[i]
        with jax.named_scope("compl%d" % i):
            sent(k, len(spots), s_recv).wait()

    def whole_latent():
        with jax.named_scope("wholelat"):
            mine = lat_own[lat_half(core), :]
            for x in range(1, nx):
                p_copy(x).wait_recv()
                mine += lat_in[x].astype(F32)
            lat[lat_half(core), :] = mine.astype(BF16)

    if n > 1:
        @pl.when(iz > 0)
        def _():
            pass_on(1)

    send_up(False, False, iz >= 0)
    for i in range(2, min(4, n)):
        pass_on(i)
    for i in range(1, min(2, n)):
        share(i)
    last = list(range(max(n - 2, min(n - 1, 1)), n))
    for i in range(1, last[0]):
        complete(i)
        @pl.when(iz >= 0)
        def _():
            halfway(order[i], 0, every)

        if i + 3 < n:
            pass_on(i + 3)
        @pl.when(iz >= 0)
        def _():
            ladder(order[i], early, True)

        share(i + 1)
        if i == last[0] - 1 and len(last) > 1:
            share(last[1])
        @pl.when(iz >= 0)
        def _():
            ladder(order[i], late, True)

    whole_latent()
    l_copy(core).start()
    if last[0] == 1 and len(last) > 1:
        share(last[1])
    for place, i in enumerate(last):
        if i > 0:
            complete(i)
            @pl.when(iz >= 0)
            def _():
                halfway(order[i], 2 - len(last) + place, every)
    l_copy(core ^ 1).wait_recv()
    @pl.when(iz >= 0)
    def _():
        finish([order[i] for i in last])

    with jax.named_scope("tail"):
        for k in range(1, n):
            sent(k, 2 * len(spots), sends).wait()
        for x in range(1, nx):
            p_copy(x).wait_send()
        l_copy(core).wait_send()


def shards(n, nj, grps, doubles, aux_factors, cycle_factors):
    _, pairs_j, width, _ = doubles.shape
    rank = cycle_factors.shape[2]
    nx = nj // CORES
    ny = grps if width % (grps * nj * 16) == 0 else 1
    others = max(n - 1, 1)
    dma = pltpu.SemaphoreType.DMA
    flag = pltpu.SemaphoreType.REGULAR
    hbm = pl.BlockSpec(memory_space=pltpu.HBM)
    flops = 4 * n * pairs_j * width**3 + 4 * pairs_j * width * width * rank
    return pl.pallas_call(
        functools.partial(sigma_kernel, n, nj, ny),
        out_shape=pltpu.VMEM(doubles.shape, BF16),
        in_specs=[hbm] * 3,
        out_specs=pl.BlockSpec(memory_space=pltpu.VMEM),
        scratch_shapes=[
            pltpu.VMEM((pairs_j, width, width), BF16),
            pltpu.VMEM((pairs_j, width, rank), BF16),
            pltpu.VMEM((n, width, width), BF16),
            pltpu.VMEM((2 * width + rank, pairs_j * width), BF16),
            pltpu.VMEM((width, pairs_j * width), F32),
            pltpu.VMEM((width, rank), BF16),
            pltpu.VMEM((width, rank), F32),
            pltpu.VMEM((width, rank), BF16),
            pltpu.VMEM((nx, width // CORES, rank), BF16),
            pltpu.VMEM((width, rank), BF16),
            dma((2,)), dma((pairs_j,)),
            flag((others,)), flag((max(nx - 1, 1),)), flag((max(ny - 1, 1),)), flag,
            dma((others,)), dma((others,)), dma((others,)), dma((others,)),
            dma((nx,)), dma((nx,)),
            dma, dma,
        ],
        compiler_params=pltpu.CompilerParams(
            collective_id=0, has_side_effects=True, vmem_limit_bytes=67043328 - doubles.size * 2 - 2**16),
        cost_estimate=pl.CostEstimate(
            flops=flops, bytes_accessed=4 * doubles.size, transcendentals=0),
    )(doubles, aux_factors, cycle_factors)


def solution(mesh):
    in_specs = (P(("grp", "ia"), "ja", None, None), P("ia", None, None), P())
    out_specs = P(("grp", "ia"), "ja", None, None)
    body = functools.partial(shards, mesh.shape["ia"], mesh.shape["ja"], mesh.shape["grp"])
    return jax.shard_map(body, mesh=mesh, in_specs=in_specs, out_specs=out_specs, check_vma=False)
```
